32 devices in a mesh: vocab: 8 (over z, y), layer: 4 (over x, core).
Axes of the slice: x: 2, y: 2, z: 4, core: 2. Of those that a mesh axis runs over, the one named last changes fastest.
Arguments:
- residual: bfloat16 [1024, 8192], P('layer', 'vocab'), may hold values from -40 to 40
- gain: bfloat16 [1, 8192], P(None, 'vocab'), may hold values from 0.25 to 1.75
- unembed: bfloat16 [8192, 128256], P(None, ('vocab', 'layer')), may hold values from -0.22097087 to 0.22097087
Outputs:
- log_probs: float32 [1024, 128256], P('layer', 'vocab')
The draws below stay inside these ranges and needn't reach their ends.
All inputs are finite; a program needn't handle non-finite values.
Results may differ from the reference program's by a relative error of at most 0.0003.
Values may be sent and summed in bfloat16 or wider, within the bound.
A program may use at most 192 MiB of HBM per device.

```python
import math
import jax
import jax.numpy as jnp
from jax import lax

D = 8192
VOCAB = 128256
TOK = 16
ROWS = 1024


def loud_offset(key):
    return jax.random.randint(jax.random.fold_in(key, 103), (), 0, 32)


def column_of(key, column):
    gaussian = jax.random.truncated_normal(jax.random.fold_in(jax.random.fold_in(key, 101), column), -4.0, 4.0, (D,), jnp.float32)
    spread = jax.random.uniform(jax.random.fold_in(jax.random.fold_in(key, 102), column), (), jnp.float32, -0.5, 0.5)
    loud = jnp.where(column % 32 == loud_offset(key), max(1.0, 80.0 / math.sqrt(D)), 1.0)
    return gaussian * (3.0 * jnp.exp(spread) * loud / math.sqrt(D))


def unit_column(key, column):
    vector = column_of(key, column)
    return vector / jnp.sqrt(jnp.mean(vector * vector))


def draw_unembed(key, part):
    columns = jax.vmap(lambda column: column_of(key, column))(jnp.arange(VOCAB))
    return columns.T.astype(jnp.bfloat16)


def draw_residual(key, part):
    offset = loud_offset(key)
    first = offset + 32 * jax.random.randint(jax.random.fold_in(key, 203), (ROWS,), 0, VOCAB // 32)
    second = offset + 32 * jax.random.randint(jax.random.fold_in(key, 204), (ROWS,), 0, VOCAB // 32)
    aligned = jax.vmap(lambda column: unit_column(key, column))(first)
    aligned = aligned + 0.99 * jax.vmap(lambda column: unit_column(key, column))(second)
    chosen = (jnp.arange(ROWS) % TOK == 0)[:, None]
    noise = jax.random.truncated_normal(jax.random.fold_in(key, 201), -4.0, 4.0, (ROWS, D), jnp.float32)
    scales = jnp.exp(jax.random.uniform(jax.random.fold_in(key, 202), (ROWS, 1), jnp.float32, 0.0, math.log(10.0)))
    strength = jnp.exp(jax.random.uniform(jax.random.fold_in(key, 205), (ROWS, 1), jnp.float32, math.log(0.2), math.log(2.0)))
    mixed = jnp.where(chosen, strength * (aligned + 0.1 * noise), noise * scales)
    return mixed.astype(jnp.bfloat16)


def setup_inputs(seed: int = 0) -> dict:
    key_of = jax.random.split(jax.random.key(seed), 4)
    residual = draw_residual(jax.random.fold_in(key_of[3], 71), 0)
    gain = jnp.clip(1.0 + 0.15 * jax.random.normal(key_of[1], (1, D), jnp.float32), 0.25, 1.75).astype(jnp.bfloat16)
    unembed = draw_unembed(jax.random.fold_in(key_of[3], 71), 0)
    return dict(residual=residual, gain=gain, unembed=unembed)


def reference(residual, gain, unembed):
    widened = residual.astype(jnp.float32)
    inverse = lax.rsqrt(lax.optimization_barrier(jnp.sum(widened * widened, axis=1)) / D + 1e-05)
    scaled = (widened * gain.astype(jnp.float32)).astype(jnp.bfloat16)
    logits = jnp.dot(scaled, unembed, preferred_element_type=jnp.float32) * inverse[:, None]
    highest = lax.optimization_barrier(jnp.max(logits, axis=1, keepdims=True))
    lse = highest + jnp.log(lax.optimization_barrier(jnp.sum(jnp.exp(logits - highest), axis=1, keepdims=True)))
    return logits - lse
```

```python
import functools

import jax
import jax.numpy as jnp
from jax import lax
from jax.experimental import pallas as pl
from jax.experimental.pallas import tpu as pltpu
from jax.sharding import PartitionSpec as P


BLOCK = 256
SLOTS = 3
HALF = 128
LOW = -1e30


def fits(residual, unembed):
    vocabs, layers = lax.axis_size("vocab"), lax.axis_size("layer")
    rows, depth = residual.shape
    columns = unembed.shape[1]
    resident = layers * rows * depth * vocabs * 2 + SLOTS * BLOCK * depth * vocabs * 2
    return (
        layers == 4
        and vocabs >= 4
        and vocabs & (vocabs - 1) == 0
        and rows == 2 * HALF
        and depth % 128 == 0
        and columns % 8 == 0
        and columns > 4 * BLOCK
        and resident + columns * 48 * HALF < 56 * 2**20
    )


def lens_kernel(
    scaled, squares, weights,
    far, near, centres, lse,
    rows_of, tiles, far_out, near_out, centre_out, sums, inverses, scales, heads, group, joined, accumulated,
    own_sem, tile_sem, near_sem,
    x_send, x_recv, hop_send, hop_recv, c_send, c_recv,
    sum_send, sum_recv, inv_send, inv_recv, far_send, far_recv, near_send, near_recv,
    cen_send, cen_recv, grp_send, grp_recv, join_send, join_recv,
):
    v, l = lax.axis_index("vocab"), lax.axis_index("layer")
    vocabs, depth = rows_of.shape[1], rows_of.shape[3]
    columns = weights.shape[0]
    width = depth * vocabs
    blocks = -(-columns // BLOCK)
    last = columns - (blocks - 1) * BLOCK
    steps = 4 * blocks
    half = vocabs // 2
    place = v // 2 + lax.rem(v, 2) * (vocabs - 1 - 2 * (v // 2))

    def remote(src, dst, send, recv, dv=0, dl=0):
        return pltpu.make_async_remote_copy(
            src_ref=src, dst_ref=dst, send_sem=send, recv_sem=recv,
            device_id={"vocab": lax.bitwise_xor(v, dv), "layer": lax.bitwise_xor(l, dl)},
            device_id_type=pl.DeviceIdType.MESH,
        )

    def mine(u, block):
        return rows_of.at[u, block, pl.ds(0, HALF)]

    def x_copy(u):
        return remote(mine(u + 2, v), mine(u, v), x_send.at[u], x_recv.at[u], dl=2)

    def seat(offset):
        turn = lax.rem(place + offset + vocabs, vocabs)
        return 2 * turn + (turn // half) * (2 * (vocabs - 1 - turn) + 1 - 2 * turn)

    def piece(h, way):
        if h < half:
            return 0, HALF
        return (0, HALF // 2) if way > 0 else (HALF // 2, HALF // 2)

    def hop(u, h, way):
        start, size = piece(h, way)
        block = rows_of.at[u, seat(-way * (h - 1)), pl.ds(start, size)]
        sems = (h - 1) if way > 0 else half + h - 1
        return pltpu.make_async_remote_copy(
            src_ref=block, dst_ref=block, send_sem=hop_send.at[u, sems], recv_sem=hop_recv.at[u, sems],
            device_id={"vocab": seat(way), "layer": l}, device_id_type=pl.DeviceIdType.MESH,
        )

    def c_copy(u, h, way):
        block = seat(-way * h)
        start, size = piece(h, way)
        sems = h if way >= 0 else half + h
        return remote(
            rows_of.at[u, block, pl.ds(start, size)], rows_of.at[u, block, pl.ds(HALF + start, size)],
            c_send.at[u, sems], c_recv.at[u, sems], dl=1,
        )

    def begin(u):
        for way in (1, -1):
            hop(u, 1, way).start()
        c_copy(u, 0, 0).start()

    def relay(u, h):
        for way in (1, -1):
            hop(u, h, way).wait_recv()
            if h < half:
                hop(u, h + 1, way).start()
            c_copy(u, h, way).start()

    def shared(u):
        return [c_copy(u, 0, 0)] + [c_copy(u, h, way) for h in range(1, half + 1) for way in (1, -1)]

    def tile_copy(g, start):
        i, slot = lax.rem(g, blocks), lax.rem(g, SLOTS)

        @pl.when(i < blocks - 1)
        def _():
            copy = pltpu.make_async_copy(
                weights.at[pl.ds(pl.multiple_of(i * BLOCK, BLOCK), BLOCK)], tiles.at[slot], tile_sem.at[slot]
            )
            copy.start() if start else copy.wait()

        @pl.when(i == blocks - 1)
        def _():
            copy = pltpu.make_async_copy(
                weights.at[pl.ds((blocks - 1) * BLOCK, last)], tiles.at[slot, pl.ds(0, last)], tile_sem.at[slot]
            )
            copy.start() if start else copy.wait()

    def far_copy(p, d, start, size):
        return remote(
            far_out.at[p, d, pl.ds(start, size)], far.at[d, p, pl.ds(start, size)],
            far_send.at[p, d], far_recv.at[p, d], dl=2 + d,
        )

    def near_copies(h, start, size):
        here = pltpu.make_async_copy(
            near_out.at[h + 2, 0, pl.ds(start, size)], near.at[0, h, pl.ds(start, size)], near_sem.at[h]
        )
        there = remote(
            near_out.at[h + 2, 1, pl.ds(start, size)], near.at[1, h, pl.ds(start, size)],
            near_send.at[h], near_recv.at[h], dl=1,
        )
        return here, there

    def send_far(b):
        p, i = b // blocks, lax.rem(b, blocks)
        start = pl.multiple_of(i * BLOCK, BLOCK)

        @pl.when(i < blocks - 1)
        def _():
            for d in range(2):
                far_copy(p, d, start, BLOCK).start()

        @pl.when(i == blocks - 1)
        def _():
            for d in range(2):
                far_copy(p, d, (blocks - 1) * BLOCK, last).start()

    def send_near(b):
        h, i = b // blocks - 2, lax.rem(b, blocks)
        start = pl.multiple_of(i * BLOCK, BLOCK)

        @pl.when(i < blocks - 1)
        def _():
            for copy in near_copies(h, start, BLOCK):
                copy.start()

        @pl.when(i == blocks - 1)
        def _():
            for copy in near_copies(h, (blocks - 1) * BLOCK, last):
                copy.start()

    def cen_copy(p, d):
        return remote(centre_out.at[p, d], centres.at[d, p], cen_send.at[p, d], cen_recv.at[p, d], dl=2 + d)

    def grp_copy(s):
        return remote(group.at[s, 0], group.at[s, 1], grp_send.at[s], grp_recv.at[s], dl=s)

    def join_copy(j):
        return remote(joined.at[0], joined.at[j], join_send.at[j], join_recv.at[j], dv=j)

    def sum_copy(j):
        return remote(squares, sums.at[j], sum_send.at[j], sum_recv.at[j], dv=j)

    def inv_copy(s):
        return remote(inverses.at[0], inverses.at[s], inv_send.at[s], inv_recv.at[s], dl=s)

    def pack(s):
        p, lanes = (0, s - 2) if s >= 2 else (2, s)
        for h in range(2):
            for r in range(2):
                group[s, 0, 2 * r + h : 2 * r + h + 1] = heads[p + h, r : r + 1, lanes * HALF : (lanes + 1) * HALF]

    for g in range(SLOTS - 1):
        tile_copy(g, True)
    owns = [
        pltpu.make_async_copy(scaled.at[pl.ds(h * HALF, HALF)], mine(2 + h, v), own_sem.at[h]) for h in range(2)
    ]
    for copy in owns:
        copy.start()
    for copy in owns:
        copy.wait()

    barrier = pltpu.get_barrier_semaphore()
    for j in range(1, vocabs):
        pl.semaphore_signal(
            barrier, inc=1, device_id={"vocab": lax.bitwise_xor(v, j), "layer": l},
            device_id_type=pl.DeviceIdType.MESH,
        )
    for s in range(1, 4):
        pl.semaphore_signal(
            barrier, inc=1, device_id={"vocab": v, "layer": lax.bitwise_xor(l, s)},
            device_id_type=pl.DeviceIdType.MESH,
        )
    pl.semaphore_wait(barrier, vocabs + 2)

    x_copy(0).start()
    x_copy(1).start()
    for j in range(1, vocabs):
        sum_copy(j).start()
    for j in range(1, vocabs):
        sum_copy(j).wait_recv()
    total = squares[...]
    for j in range(1, vocabs):
        total = total + sums[j]
    inverses[0] = lax.rsqrt(total / width + 1e-05)

    x_copy(0).wait_recv()
    begin(0)
    for s in range(1, 4):
        inv_copy(s).start()
    x_copy(1).wait_recv()
    begin(1)
    for h in range(1, half):
        relay(0, h)
    relay(1, 1)
    begin(2)
    for s in range(1, 4):
        inv_copy(s).wait_recv()
    for p in range(4):
        for lanes in range(2):
            s = lanes if p >= 2 else 2 + lanes
            scales[p, 0:1, lanes * HALF : (lanes + 1) * HALF] = inverses[s, p % 2 : p % 2 + 1]
    relay(0, half)
    order = [(0, h) for h in range(2, half)] + [(1, 1), (0, half)]
    when = [3, 9, 10, 14][: len(order)]

    def absorb(g, highest, totals):
        p, i = g // blocks, lax.rem(g, blocks)
        logits = accumulated[...] * scales[p, 0:1]
        count = jnp.minimum(columns - i * BLOCK, BLOCK)
        inside = lax.broadcasted_iota(jnp.int32, logits.shape, 0) < count
        shown = jnp.where(inside, logits, LOW)
        highest = jnp.where(i == 0, LOW, highest)
        totals = jnp.where(i == 0, 0.0, totals)
        top = jnp.maximum(highest, jnp.max(shown, axis=0, keepdims=True))
        totals = totals * jnp.exp(highest - top) + jnp.sum(jnp.exp(shown - top), axis=0, keepdims=True)
        heads[p, 0:1] = top
        heads[p, 1:2] = totals
        start = pl.multiple_of(i * BLOCK, BLOCK)
        centre = jnp.sum(jnp.where(inside, logits, 0.0), axis=0, keepdims=True) / count.astype(jnp.float32)
        short = (logits - centre).astype(jnp.bfloat16)
        for d in range(2):
            lanes = slice(d * HALF, (d + 1) * HALF)
            centre_out[p, d, pl.ds(i, 1)] = centre[:, lanes]
            far_out[p, d, pl.ds(start, BLOCK)] = short[:, lanes]
            near_out[p, d, pl.ds(start, BLOCK)] = logits[:, lanes]
        return top, totals

    def step(g, carry):
        p, i = g // blocks, lax.rem(g, blocks)
        u = p + 1

        @pl.when(i == 0)
        def _():
            for copy in shared(p):
                copy.wait_recv()

        @pl.when(g == 2 * blocks + 1)
        def _():
            for s in range(2, 4):
                pack(s)

        @pl.when(g == 2 * blocks + 2)
        def _():
            for s in range(2, 4):
                grp_copy(s).start()
            for q in range(2):
                for d in range(2):
                    cen_copy(q, d).start()

        for (later, h), at in zip(order, when):

            @pl.when((i == at) & (u + later < 4))
            def _(later=later, h=h):
                relay(u + later, h)
                if later:

                    @pl.when(u + later < 3)
                    def _():
                        begin(u + later + 1)

        upto, before = jnp.minimum((g - 1) * 5 // 9, 2 * blocks), jnp.minimum((g - 2) * 5 // 9, 2 * blocks)

        @pl.when((g > 1) & (upto > before))
        def _():
            send_far(before)

        @pl.when(g > 2 * blocks + 1)
        def _():
            send_near(g - 2)

        tile_copy(g, False)

        @pl.when(g + SLOTS - 1 < steps)
        def _():
            tile_copy(g + SLOTS - 1, True)

        carry = absorb(jnp.maximum(g - 1, 0), *carry)
        slot = lax.rem(g, SLOTS)
        product = None
        for b in range(vocabs):
            part = lax.dot_general(
                tiles[slot, :, b * depth : (b + 1) * depth], rows_of[p, b],
                (((1,), (1,)), ((), ())), preferred_element_type=jnp.float32,
            )
            product = part if product is None else product + part
        accumulated[...] = product
        return carry

    zero = jnp.zeros((1, 2 * HALF), jnp.float32)
    accumulated[...] = jnp.zeros_like(accumulated)
    carry = lax.fori_loop(0, steps, step, (zero, zero))
    send_near(jnp.int32(steps - 2))
    absorb(jnp.int32(steps - 1), *carry)

    for s in range(2):
        pack(s)
    send_near(jnp.int32(steps - 1))
    grp_copy(1).start()

    def join(a, b):
        top = jnp.maximum(a[0:2], b[0:2])
        return jnp.concatenate([top, a[2:4] * jnp.exp(a[0:2] - top) + b[2:4] * jnp.exp(b[0:2] - top)], axis=0)

    best = group[0, 0, 0:4]
    for s in range(1, 4):
        grp_copy(s).wait_recv()
        best = join(best, group[s, 1, 0:4])
    joined[0, 0:4] = best
    for h in range(2):
        here, there = near_copies(h, 0, columns)
        here.wait()
        there.wait_send()
    for j in range(1, vocabs):
        join_copy(j).start()
    for j in range(1, vocabs):
        join_copy(j).wait_recv()
        best = join(best, joined[j, 0:4])
    lse[...] = jnp.zeros_like(lse)
    lse[0:2] = best[0:2] + jnp.log(best[2:4])

    for h in range(2):
        near_copies(h, 0, columns)[1].wait_recv()
    for q in range(2):
        for d in range(2):
            cen_copy(q, d).wait()
            far_copy(q, d, 0, columns).wait()
    for u in range(2):
        x_copy(u).wait_send()

    def drain(u, none):
        for h in range(1, half + 1):
            for way in (1, -1):
                hop(u, h, way).wait_send()
        for copy in shared(u):
            copy.wait_send()
        return none

    lax.fori_loop(0, 4, drain, 0)
    for j in range(1, vocabs):
        sum_copy(j).wait_send()
        join_copy(j).wait_send()
    for s in range(1, 4):
        inv_copy(s).wait_send()
        grp_copy(s).wait_send()


def finish_kernel(blocks, far, near, centres, lse, out):
    me, j = lax.axis_index("layer"), pl.program_id(0)
    for s in range(4):
        slot = lax.bitwise_xor(me, s)
        for h in range(2):
            lanes = slice(h * HALF, (h + 1) * HALF)
            shift = lse[h : h + 1]
            if s < 2:
                out[slot, :, lanes] = near[s, h] - shift
                continue
            for b in range(blocks):
                rows = slice(b * BLOCK, (b + 1) * BLOCK)
                centre = centres[s - 2, h, pl.ds(j * blocks + b, 1)]
                out[slot, rows, lanes] = far[s - 2, h, rows].astype(jnp.float32) + (centre - shift)


def streamed(residual, gain, unembed):
    vocabs = lax.axis_size("vocab")
    rows, depth = residual.shape
    columns = unembed.shape[1]
    blocks = -(-columns // BLOCK)
    padded = blocks * BLOCK

    widened = residual.astype(jnp.float32)
    squares = jnp.sum(widened * widened, axis=1).reshape(2, HALF)
    squares = jnp.concatenate([squares, jnp.ones((6, HALF), jnp.float32)], axis=0)
    scaled = (widened * gain.astype(jnp.float32)).astype(jnp.bfloat16)

    f32, bf16 = jnp.float32, jnp.bfloat16
    dma = pltpu.SemaphoreType.DMA
    hbm, vmem = pl.BlockSpec(memory_space=pltpu.HBM), pl.BlockSpec(memory_space=pltpu.VMEM)
    far, near, centres, lse = pl.pallas_call(
        lens_kernel,
        out_shape=(
            jax.ShapeDtypeStruct((2, 2, columns, HALF), bf16),
            jax.ShapeDtypeStruct((2, 2, columns, HALF), f32),
            jax.ShapeDtypeStruct((2, 2, blocks, HALF), f32),
            jax.ShapeDtypeStruct((8, HALF), f32),
        ),
        in_specs=[hbm, vmem, hbm],
        out_specs=(hbm, hbm, hbm, vmem),
        scratch_shapes=[
            pltpu.VMEM((4, vocabs, 2 * HALF, depth), bf16),
            pltpu.VMEM((SLOTS, BLOCK, depth * vocabs), bf16),
            pltpu.VMEM((4, 2, padded, HALF), bf16),
            pltpu.VMEM((4, 2, padded, HALF), f32),
            pltpu.VMEM((4, 2, blocks, HALF), f32),
            pltpu.VMEM((vocabs, 8, HALF), f32),
            pltpu.VMEM((4, 8, HALF), f32),
            pltpu.VMEM((4, 8, 2 * HALF), f32),
            pltpu.VMEM((4, 8, 2 * HALF), f32),
            pltpu.VMEM((4, 2, 8, HALF), f32),
            pltpu.VMEM((vocabs, 8, HALF), f32),
            pltpu.VMEM((BLOCK, 2 * HALF), f32),
            dma((2,)), dma((SLOTS,)), dma((2,)),
            dma((2,)), dma((2,)), dma((4, vocabs)), dma((4, vocabs)),
            dma((4, vocabs + 1)), dma((4, vocabs + 1)),
            dma((vocabs,)), dma((vocabs,)), dma((4,)), dma((4,)), dma((2, 2)), dma((2, 2)), dma((2,)), dma((2,)),
            dma((2, 2)), dma((2, 2)), dma((4,)), dma((4,)), dma((vocabs,)), dma((vocabs,)),
        ],
        compiler_params=pltpu.CompilerParams(
            collective_id=0, has_side_effects=True, vmem_limit_bytes=62 * 2**20
        ),
        cost_estimate=pl.CostEstimate(
            flops=2 * 4 * rows * columns * depth * vocabs,
            bytes_accessed=4 * columns * depth * vocabs * 2,
            transcendentals=4 * rows * columns,
        ),
        name="lens",
    )(scaled, squares, unembed.T)

    tile = 4 * BLOCK
    out = pl.pallas_call(
        functools.partial(finish_kernel, tile // BLOCK),
        out_shape=jax.ShapeDtypeStruct((4, columns, rows), f32),
        grid=(-(-columns // tile),),
        in_specs=[
            pl.BlockSpec((2, 2, tile, HALF), lambda j: (0, 0, j, 0)),
            pl.BlockSpec((2, 2, tile, HALF), lambda j: (0, 0, j, 0)),
            pl.BlockSpec((2, 2, blocks, HALF), lambda j: (0, 0, 0, 0)),
            pl.BlockSpec((8, HALF), lambda j: (0, 0)),
        ],
        out_specs=pl.BlockSpec((4, tile, rows), lambda j: (0, j, 0)),
        compiler_params=pltpu.CompilerParams(vmem_limit_bytes=62 * 2**20),
        name="finish",
    )(far, near, centres, lse)
    return out.reshape(4 * columns, rows).T


def to_partner(value, step, size):
    return lax.ppermute(value, "layer", [(l, l ^ step) for l in range(size)])


def ring_of(size):
    return list(range(0, size, 2)) + list(range(1, size, 2))[::-1]


def ring_gather(block, place):
    size = lax.axis_size("vocab")
    ring = ring_of(size)
    order = jnp.array(ring, jnp.int32)
    where = jnp.array([ring.index(v) for v in range(size)], jnp.int32)[lax.axis_index("vocab")]
    up = [(ring[p], ring[(p + 1) % size]) for p in range(size)]
    down = [(b, a) for a, b in up]
    half, rows = size // 2, block.shape[0]
    place(block, order[where], 0)
    forward = backward = block
    for k in range(1, half + 1):
        if k == half and size % 2 == 0:
            forward, backward = forward[: rows // 2], backward[rows // 2 :]
        forward = lax.ppermute(forward, "vocab", up)
        backward = lax.ppermute(backward, "vocab", down)
        if k == max(half - 1, 1):
            nearly = (forward, backward)
        place(forward, order[(where - k) % size], 0)
        place(backward, order[(where + k) % size], rows - backward.shape[0])
    return nearly


def local(residual, gain, unembed):
    if fits(residual, unembed):
        return streamed(residual, gain, unembed)
    return body(residual, gain, unembed)


def body(residual, gain, unembed):
    layers = lax.axis_size("layer")
    vocabs = lax.axis_size("vocab")
    rows, depth = residual.shape
    columns = unembed.shape[1]
    me = lax.axis_index("layer")
    width = depth * vocabs

    widened = residual.astype(jnp.float32)
    squares = jnp.sum(widened * widened, axis=1)
    scaled = (widened * gain.astype(jnp.float32)).astype(jnp.bfloat16)

    total = lax.all_gather(squares, "vocab").sum(0)
    own_inverse = lax.rsqrt(total / width + 1e-05)
    inverse = [to_partner(own_inverse, s, layers) if s else own_inverse for s in range(layers)]

    evens = [s for s in range(layers - 2, -1, -2)] if layers > 1 else [0]
    firsts = {s: to_partner(scaled, s, layers) if s else scaled for s in evens}
    full = {}
    after = own_inverse
    for step in evens:
        first, _ = lax.optimization_barrier((firsts[step], after))
        if step == 0:
            full[0] = lax.all_gather(first, "vocab", axis=1, tiled=True)
            break
        steps = [step, step + 1] if layers > 1 else [step]
        for s in steps:
            full[s] = jnp.zeros((rows, width), jnp.bfloat16)

        def place(block, owner, row):
            column = owner * depth
            full[step] = lax.dynamic_update_slice(full[step], block, (row, column))
            if layers > 1:
                other = to_partner(block, 1, layers)
                full[step + 1] = lax.dynamic_update_slice(full[step + 1], other, (row, column))

        after = ring_gather(first, place)

    order = [s for e in evens for s in ([e, e + 1] if layers > 1 else [e])]
    sent, heads = {}, {}
    for at, step in enumerate(order):
        inv = inverse[step]
        if step == 0 and layers > 1:
            full[1] = to_partner(full[0], 1, layers)
        products = lax.dot_general(unembed, full[step], (((0,), (1,)), ((), ())), preferred_element_type=jnp.float32)
        logits = products * inv[None, :]
        highest = jnp.max(logits, axis=0)
        centre = jnp.mean(logits, axis=0)
        totals = jnp.sum(jnp.exp(logits - highest[None, :]), axis=0)
        head = jnp.stack([highest, totals, centre])
        if step:
            heads[step] = to_partner(head, step, layers)
            short = (logits - centre[None, :]).astype(jnp.float16)
            if at + 1 < len(order) and order[at + 1] in full:
                following = order[at + 1]
                short, full[following] = lax.optimization_barrier((short, full[following]))
            sent[step] = to_partner(short, step, layers)
        else:
            heads[step] = head
            sent[step] = logits

    mine = jnp.stack([heads[s] for s in range(layers)])
    everyone = lax.all_gather(mine, "vocab")
    highest = jnp.max(everyone[:, :, 0], axis=(0, 1))
    totals = jnp.sum(everyone[:, :, 1] * jnp.exp(everyone[:, :, 0] - highest), axis=(0, 1))
    lse = highest + jnp.log(totals)

    out = jnp.zeros((layers, columns, rows), jnp.float32)
    for step in [0] + [s for s in order[::-1] if s]:
        if step:
            value = sent[step].astype(jnp.float32) + (mine[step, 2] - lse)[None, :]
        else:
            value = sent[step] - lse[None, :]
        out = lax.dynamic_update_slice(out, value[None], (me ^ step, 0, 0))
    return out.reshape(layers * columns, rows).T


def solution(mesh):
    placed = (P("layer", "vocab"), P(None, "vocab"), P(None, ("vocab", "layer")))
    return jax.shard_map(
        local, mesh=mesh, in_specs=placed, out_specs=P("layer", "vocab"), check_vma=False
    )
```
